32 devices in a mesh: groups: 2 (over y), fsdp: 4 (over z), expert: 4 (over x, core).
Axes of the slice: x: 2, y: 2, z: 4, core: 2. Of those that a mesh axis runs over, the one named last changes fastest.
Arguments:
- queries: bfloat16 [512, 2048], P(('groups', 'fsdp'), 'expert'), parts along dimension 0, may hold values from -14 to 14
- keys: bfloat16 [8, 2048, 512], P(('groups', 'fsdp'), None, 'expert'), parts along dimension 0, may hold values from -14 to 14
- values: bfloat16 [8, 2048, 512], P(('groups', 'fsdp'), None, 'expert'), parts along dimension 0, may hold values from -4 to 4
- out_weight: bfloat16 [2048, 4096], P('expert', 'fsdp'), may hold values from -0.5 to 0.5
- residual: bfloat16 [512, 4096], P(('groups', 'fsdp')), parts along dimension 0, may hold values from -3 to 3
- norm_gain: float32 [4096], replicated, may hold values from 0.5 to 1.5
- route_ids: int32 [512, 2], P(('groups', 'fsdp')), parts along dimension 0, may hold values from 0 to 7, as said below
- route_slots: int32 [512, 2], P(('groups', 'fsdp')), parts along dimension 0, may hold values from 0 to 23, as said below
- route_weights: int32 [512, 2], P(('groups', 'fsdp')), parts along dimension 0, may hold values from 1 to 65535, as said below
- w_gate: bfloat16 [8, 4096, 7168], P('expert', None, 'fsdp'), may hold values from -0.09375 to 0.09375
- w_up: bfloat16 [8, 4096, 7168], P('expert', None, 'fsdp'), may hold values from -0.09375 to 0.09375
- w_down: bfloat16 [8, 7168, 4096], P('expert', 'fsdp'), may hold values from -0.0625 to 0.0625
Outputs:
- layer_out: bfloat16 [512, 4096], P(('groups', 'fsdp'), 'expert'), parts along dimension 0
The draws below stay inside these ranges and needn't reach their ends.
There are 2 independent parts, one for each index of `groups`. The reference program is written for one: setup_inputs(seed, part) draws one part's arguments, and reference() takes and returns one part's arrays. A program takes and returns all parts, laid end to end along the dimension named above; an argument that names none is the same for every part. Nothing has to cross between parts.
Inputs may be any that keep to these rules, and one draw needn't show every extreme that they name: `route_ids`: each row names two different experts. Among the rows of one block, no expert is named more than 24 times and no group of experts 2 g and 2 g + 1 more than 36 times; one expert, the same for all blocks, is named exactly 24 times in every block and its group exactly 36 times; every expert is named in every block. `route_slots`: within one block, the routes to one expert hold the slots 0 to their count - 1, each once. `route_weights`: the two entries of a row sum to 65536.
All inputs are finite; a program needn't handle non-finite values.
Results may differ from the reference program's by a relative error of at most 0.02.
Values may be sent and summed in bfloat16 or wider, within the bound.
No kernel may reach another device: no remote copies, remote signals or barrier semaphores. Data moves between devices by JAX's collectives and lax.ppermute only.
A program may use at most 192 MiB of HBM per device.

```python
import jax
import jax.numpy as jnp
from jax import lax

D = 4096
HEADS = 16
KV_HEADS = 4
HEAD_DIM = 128
EXPERTS = 8
FFW = 7168
Q_BLOCK = 64
CTX = 2048
CAP = 24
GCAP = 36
SEQS = 4
TOKENS = 256
N_FSDP = 4


def draw_queries(key, part):
    base_key = jax.random.fold_in(key, 5)
    shape = (SEQS, Q_BLOCK, KV_HEADS, HEADS // KV_HEADS, HEAD_DIM)
    base = jnp.clip(1.5 * jax.random.normal(base_key, shape, jnp.float32), -6.0, 6.0)
    return base.reshape(TOKENS, HEADS * HEAD_DIM).astype(jnp.bfloat16)


def draw_keys(key, part):
    base_key = jax.random.fold_in(key, 6)
    shape = (SEQS, CTX, KV_HEADS, HEAD_DIM)
    base = jnp.clip(jax.random.normal(base_key, shape, jnp.float32), -4.0, 4.0)
    return base.reshape(SEQS, CTX, KV_HEADS * HEAD_DIM).astype(jnp.bfloat16)


def shuffle_one(key):
    return jax.random.permutation(key, Q_BLOCK)


def route_table(key):
    sub = jax.random.fold_in(key, 11)
    busy_key, sum_key, turn_key, split_key, order_key = jax.random.split(sub, 5)
    busy = jax.random.randint(busy_key, (), 0, EXPERTS)
    busy_pair = busy // 2
    lower = 7 * Q_BLOCK // 16
    drawn = jax.random.randint(sum_key, (SEQS, 2), lower, GCAP + 1)
    third = 2 * Q_BLOCK - GCAP - drawn[:, 0] - drawn[:, 1]
    others = jnp.concatenate([drawn, third[:, None]], axis=1)
    turn = jax.random.randint(turn_key, (SEQS, 1), 0, 3)
    others = jnp.take_along_axis(others, (jnp.arange(3)[None, :] + turn) % 3, axis=1)
    pairs = jnp.arange(EXPERTS // 2)
    other_index = jnp.clip(pairs - (pairs > busy_pair).astype(jnp.int32), 0, 2)
    pair_sums = jnp.where(pairs[None, :] == busy_pair, GCAP, jnp.take(others, other_index, axis=1))
    low_split = jnp.maximum(pair_sums - CAP, 1)
    high_split = jnp.minimum(pair_sums - 1, CAP)
    evens = jax.random.randint(split_key, (SEQS, EXPERTS // 2), low_split, high_split + 1)
    busy_even = jnp.where(busy % 2 == 0, CAP, GCAP - CAP)
    evens = jnp.where(pairs[None, :] == busy_pair, busy_even, evens)
    counts = jnp.stack([evens, pair_sums - evens], axis=2).reshape(SEQS, EXPERTS)
    ends = jnp.cumsum(counts, axis=1)
    starts = ends - counts
    position = jnp.arange(2 * Q_BLOCK)
    owner = jnp.sum((ends[:, None, :] <= position[None, :, None]).astype(jnp.int32), axis=2)
    rank = position[None, :] - jnp.take_along_axis(starts, owner, axis=1)
    order = jax.vmap(shuffle_one)(jax.random.split(order_key, SEQS))
    pick = jnp.stack([order, order + Q_BLOCK], axis=2).reshape(SEQS, 2 * Q_BLOCK)
    route_ids = jnp.take_along_axis(owner, pick, axis=1).reshape(TOKENS, 2)
    route_slots = jnp.take_along_axis(rank, pick, axis=1).reshape(TOKENS, 2)
    return (route_ids.astype(jnp.int32), route_slots.astype(jnp.int32))


def draw_route_ids(key, part):
    return route_table(key)[0]


def draw_route_slots(key, part):
    return route_table(key)[1]


def draw_route_weights(key, part):
    leading = jax.random.randint(jax.random.fold_in(key, 3), (TOKENS,), 1, 65536)
    return jnp.stack([leading, 65536 - leading], axis=1).astype(jnp.int32)


def levels(stream_key, shape, shards, least, top_value):
    loudness, own = 1.0, jax.random.fold_in(stream_key, 6)
    for axis_at, parts in shards:
        heights = jnp.exp(jax.random.uniform(jax.random.fold_in(own, axis_at), (parts,), jnp.float32, least / len(shards), top_value / len(shards)))
        loudness = loudness * jnp.repeat(heights, shape[axis_at] // parts).reshape([-1 if axis == axis_at else 1 for axis in range(len(shape))])
    return loudness


def normal_values(rng, extent, scale, bound, pieces=(), kind=jnp.bfloat16):
    factor_of = levels(rng, extent, pieces, -0.22, 0.18) if pieces else 1.0
    entries = jax.random.normal(rng, extent, jnp.float32) * scale * factor_of
    return jnp.minimum(jnp.maximum(entries, -bound), bound).astype(kind)


def setup_inputs(seed: int = 0, part: int = 0) -> dict:
    key_list = jax.random.split(jax.random.key(seed), 13)
    part_keys = jax.random.split(jax.random.fold_in(key_list[12], part), 13)
    return {
        "queries": draw_queries(jax.random.fold_in(jax.random.fold_in(key_list[12], part), 71), part),
        "keys": draw_keys(jax.random.fold_in(jax.random.fold_in(key_list[12], part), 71), part),
        "values": normal_values(part_keys[2], (SEQS, CTX, KV_HEADS * HEAD_DIM), 1.0, 4.0, ((0, 4), (2, 4))),
        "out_weight": normal_values(key_list[3], (HEADS * HEAD_DIM, D), HEAD_DIM ** -0.5, 0.5, ((0, 4), (1, 4))),
        "residual": normal_values(part_keys[4], (TOKENS, D), 0.5, 3.0, ((0, 4),)),
        "norm_gain": jnp.clip(1.0 + 0.1 * jax.random.normal(key_list[5], (D,), jnp.float32), 0.5, 1.5),
        "route_ids": draw_route_ids(jax.random.fold_in(jax.random.fold_in(key_list[12], part), 71), part),
        "route_slots": draw_route_slots(jax.random.fold_in(jax.random.fold_in(key_list[12], part), 71), part),
        "route_weights": draw_route_weights(jax.random.fold_in(jax.random.fold_in(key_list[12], part), 71), part),
        "w_gate": normal_values(key_list[9], (EXPERTS, D, FFW), D ** -0.5, 0.09375, ((0, 4), (2, 4))),
        "w_up": normal_values(key_list[10], (EXPERTS, D, FFW), D ** -0.5, 0.09375, ((0, 4), (2, 4))),
        "w_down": normal_values(key_list[11], (EXPERTS, FFW, D), FFW ** -0.5, 0.0625, ((0, 4), (1, 4))),
    }


eps = 1e-05

def attend_one(item):
    query_block, key_block, value_block = item
    block = query_block.shape[0]
    context = key_block.shape[0]
    group = HEADS // KV_HEADS
    query_heads = query_block.reshape(block, KV_HEADS, group, HEAD_DIM).astype(jnp.float32)
    key_heads = key_block.reshape(context, KV_HEADS, HEAD_DIM).astype(jnp.float32)
    value_heads = value_block.reshape(context, KV_HEADS, HEAD_DIM).astype(jnp.float32)
    scores = jnp.einsum('qcgd,kcd->cgqk', query_heads, key_heads) * HEAD_DIM ** (-0.5)
    key_pos = jnp.arange(context)
    query_pos = context - block + jnp.arange(block)
    allowed = key_pos[None, :] <= query_pos[:, None]
    masked = jnp.where(allowed, scores, -1e+30)
    highest = lax.optimization_barrier(jnp.max(masked, axis=-1, keepdims=True))
    weights = jnp.where(allowed, jnp.exp(masked - highest), 0.0)
    probs = (weights / lax.optimization_barrier(jnp.sum(weights, axis=-1, keepdims=True))).astype(jnp.bfloat16)
    heads_out = jnp.einsum('cgqk,kcd->qcgd', probs.astype(jnp.float32), value_heads)
    return heads_out.astype(jnp.bfloat16).reshape(block, HEADS * HEAD_DIM)

def expert_one(item):
    rows, gate_w, up_w, down_w = item
    gate = jnp.dot(rows, gate_w, preferred_element_type=jnp.float32)
    upper = jnp.dot(rows, up_w, preferred_element_type=jnp.float32)
    hidden = (jax.nn.silu(gate) * upper).astype(jnp.bfloat16)
    width = FFW // N_FSDP
    hidden_runs = hidden.reshape(rows.shape[0], N_FSDP, width).transpose(1, 0, 2)
    down_runs = down_w.reshape(N_FSDP, width, down_w.shape[1])

    def add_run(total, pair):
        part = jnp.dot(pair[0], pair[1], preferred_element_type=jnp.float32)
        part = lax.optimization_barrier(part.astype(jnp.bfloat16)).astype(jnp.float32)
        return (total + part, None)
    start_total = jnp.zeros((rows.shape[0], down_w.shape[1]), jnp.float32)
    total, unused = lax.scan(add_run, start_total, (hidden_runs, down_runs))
    return total

def reference(queries, keys, values, out_weight, residual, norm_gain, route_ids, route_slots, route_weights, w_gate, w_up, w_down):
    query_blocks = queries.reshape(SEQS, Q_BLOCK, HEADS * HEAD_DIM)
    heads_out = lax.map(attend_one, (query_blocks, keys, values)).reshape(TOKENS, HEADS * HEAD_DIM)
    attn = jnp.dot(heads_out, out_weight, preferred_element_type=jnp.float32)
    hstate = (residual.astype(jnp.float32) + attn).astype(jnp.bfloat16)
    state = hstate.astype(jnp.float32)
    scale = lax.rsqrt(lax.optimization_barrier(jnp.mean(state * state, axis=-1, keepdims=True)) + eps)
    normed = (state * scale * norm_gain).astype(jnp.bfloat16)
    block_of = (jnp.arange(TOKENS) // Q_BLOCK).astype(jnp.int32)
    spread = jnp.broadcast_to(normed[:, None, :], (TOKENS, 2, D))
    buffer = jnp.zeros((SEQS, EXPERTS, CAP, D), jnp.bfloat16)
    buffer = buffer.at[block_of[:, None], route_ids, route_slots].set(spread)
    expert_rows = buffer.transpose(1, 0, 2, 3).reshape(EXPERTS, SEQS * CAP, D)
    expert_out = lax.map(expert_one, (expert_rows, w_gate, w_up, w_down)).reshape(EXPERTS, SEQS, CAP, D)
    picked = expert_out[route_ids, block_of[:, None], route_slots]
    route_share = route_weights.astype(jnp.float32) / 65536.0
    moe = lax.optimization_barrier(jnp.sum(route_share[:, :, None] * picked, axis=1))
    return (hstate.astype(jnp.float32) + moe).astype(jnp.bfloat16)
```

```python
import jax
import jax.numpy as jnp
from jax import lax
from jax.sharding import PartitionSpec as P

HEAD_DIM = 128
GCAP = 36
ROUTE_LANES = 128

eps = 1e-05


def attend(queries, keys, values):
    block = queries.shape[0]
    context = keys.shape[1]
    kv_dev = keys.shape[2] // HEAD_DIM
    heads_dev = queries.shape[1] // HEAD_DIM
    group = heads_dev // kv_dev
    query_heads = queries.reshape(block, kv_dev, group, HEAD_DIM)
    key_heads = keys[0].reshape(context, kv_dev, HEAD_DIM)
    value_heads = values[0].reshape(context, kv_dev, HEAD_DIM)
    scores = jnp.einsum(
        "qcgd,kcd->cgqk", query_heads, key_heads, preferred_element_type=jnp.float32
    ) * HEAD_DIM ** (-0.5)
    key_pos = jnp.arange(context)
    query_pos = context - block + jnp.arange(block)
    allowed = key_pos[None, :] <= query_pos[:, None]
    masked = jnp.where(allowed, scores, -1e30)
    highest = jnp.max(masked, axis=-1, keepdims=True)
    weights = jnp.where(allowed, jnp.exp(masked - highest), 0.0)
    probs = (weights / jnp.sum(weights, axis=-1, keepdims=True)).astype(jnp.bfloat16)
    heads_out = jnp.einsum("cgqk,kcd->qcgd", probs, value_heads, preferred_element_type=jnp.float32)
    return heads_out.astype(jnp.bfloat16).reshape(block, heads_dev * HEAD_DIM)


def make_per_device(n_fsdp, n_expert):
    bits = []
    step = 1
    while step < n_expert:
        bits.append(step)
        step *= 2

    def shift(value, by):
        pairs = [(i, (i + by) % n_fsdp) for i in range(n_fsdp)]
        return lax.ppermute(value, "fsdp", pairs)

    def swap(value, bit):
        return lax.ppermute(value, "expert", [(i, i ^ bit) for i in range(n_expert)])

    def split_sum(blocks, group_index):
        for bit in bits:
            low = (group_index & bit) == 0
            pairs = [(blocks[2 * k], blocks[2 * k + 1]) for k in range(len(blocks) // 2)]
            keep = [jnp.where(low, a, b) for a, b in pairs]
            send = [jnp.where(low, b, a).astype(jnp.bfloat16) for a, b in pairs]
            got = swap(jnp.stack(send), bit)
            blocks = [a.astype(jnp.float32) + got[k].astype(jnp.float32) for k, a in enumerate(keep)]
        return blocks[0]

    def per_device(
        queries,
        keys,
        values,
        out_weight,
        residual,
        norm_gain,
        route_ids,
        route_slots,
        route_weights,
        w_gate,
        w_up,
        w_down,
    ):
        bf16, f32 = jnp.bfloat16, jnp.float32
        me = lax.axis_index("fsdp")
        group_index = lax.axis_index("expert")
        block, width = residual.shape
        tokens = n_fsdp * block
        column_run = width // n_fsdp
        quarter = column_run // n_expert

        table = jnp.concatenate(
            [route_ids, route_slots, route_weights // 256, route_weights % 256], axis=1
        ).astype(bf16)
        table = jnp.pad(table, ((0, 0), (0, ROUTE_LANES - table.shape[1])))

        def early(by):
            dest = lax.rem(me + by, n_fsdp)
            start = dest * column_run + group_index * quarter
            return jnp.concatenate(
                [lax.dynamic_slice_in_dim(residual, start, quarter, 1), table], axis=1
            )

        def place(parts):
            out = jnp.zeros((n_fsdp,) + parts[0].shape, parts[0].dtype)
            for by, part in enumerate(parts):
                source = lax.rem(me - by + n_fsdp, n_fsdp)
                out = lax.dynamic_update_slice_in_dim(out, part[None], source, 0)
            return out

        early_all = place([early(0)] + [shift(early(by), by) for by in range(1, n_fsdp)])
        residual_part = early_all[:, :, :quarter].reshape(tokens, quarter)
        routes = early_all[:, :, quarter : quarter + 8].astype(f32)

        heads_out = attend(queries, keys, values)
        heads_all = place([heads_out] + [shift(heads_out, by) for by in range(1, n_fsdp)])
        partial_attn = jnp.dot(
            heads_all.reshape(tokens, heads_out.shape[1]), out_weight, preferred_element_type=f32
        )
        blocks = [partial_attn[:, i * quarter : (i + 1) * quarter] for i in range(n_expert)]
        attn = split_sum(blocks, group_index)
        own = (residual_part.astype(f32) + attn).astype(bf16)

        def spread(piece):
            pieces = [piece]
            for bit in reversed(bits[1:]):
                low = (group_index & bit) == 0
                got = swap(jnp.stack(pieces), bit)
                pieces = [
                    part
                    for k, mine in enumerate(pieces)
                    for part in (jnp.where(low, mine, got[k]), jnp.where(low, got[k], mine))
                ]
            return jnp.concatenate(pieces, axis=1)

        chunks = place([spread(own)] + [spread(shift(own, by)) for by in range(1, n_fsdp)])
        low = (group_index & 1) == 0
        other = swap(chunks, 1) if n_expert > 1 else chunks
        even = jnp.where(low, chunks, other).reshape(n_fsdp, tokens, n_expert // 2, 1, quarter)
        odd = jnp.where(low, other, chunks).reshape(n_fsdp, tokens, n_expert // 2, 1, quarter)
        hstate = (
            jnp.concatenate([even, odd], axis=3)
            .reshape(n_fsdp, tokens, column_run)
            .transpose(1, 0, 2)
            .reshape(tokens, width)
        )

        state = hstate.astype(f32)
        scale = lax.rsqrt(jnp.mean(state * state, axis=-1, keepdims=True) + eps)
        normed = (state * scale * norm_gain).astype(bf16)

        first_expert = (2 * group_index).astype(f32)
        ids, slots = routes[:, :, 0:2], routes[:, :, 2:4]
        within = ids - first_expert
        in_group = (within >= 0) & (within < 2)
        lead_count = jnp.sum((within == 0).astype(f32), axis=(1, 2))
        row_of = jnp.arange(n_fsdp, dtype=f32)[:, None, None] * GCAP
        row_of = row_of + slots + within * lead_count[:, None, None]
        target = jnp.where(in_group, row_of, -1.0).reshape(tokens, 2)
        row_ids = jnp.arange(n_fsdp * GCAP, dtype=f32)
        hit0 = target[:, 0:1] == row_ids[None, :]
        hit1 = target[:, 1:2] == row_ids[None, :]
        pick = (hit0 | hit1).astype(bf16)
        rows = lax.dot_general(
            pick, normed, (((0,), (0,)), ((), ())), preferred_element_type=f32
        ).astype(bf16)
        in_block = row_ids - jnp.repeat(jnp.arange(n_fsdp, dtype=f32) * GCAP, GCAP)
        labels = (in_block >= jnp.repeat(lead_count, GCAP)).astype(f32)
        keep = jnp.stack([1.0 - labels, labels], axis=0)[:, :, None]
        gate = jnp.einsum("nd,edf->enf", rows, w_gate, preferred_element_type=f32)
        upper = jnp.einsum("nd,edf->enf", rows, w_up, preferred_element_type=f32)
        hidden = (jax.nn.silu(gate) * upper * keep).astype(bf16)
        expert_out = jnp.einsum(
            "enf,efd->nd", hidden, w_down, preferred_element_type=f32
        ).astype(bf16)

        parts = routes[:, :, 4:8].reshape(tokens, 4)
        zero = jnp.zeros((), f32)
        high = jnp.where(hit0, parts[:, 0:1], zero) + jnp.where(hit1, parts[:, 1:2], zero)
        less = jnp.where(hit0, parts[:, 2:3], zero) + jnp.where(hit1, parts[:, 3:4], zero)
        high = (high / 256.0).astype(bf16)
        less = (less / 65536.0).astype(bf16)
        contrib = jnp.dot(high, expert_out, preferred_element_type=f32) + jnp.dot(
            less, expert_out, preferred_element_type=f32
        )
        run = width // n_expert
        own_moe = split_sum([contrib[:, i * run : (i + 1) * run] for i in range(n_expert)], group_index)
        own_moe = own_moe.reshape(n_fsdp, block, run)

        def for_block(by):
            dest = lax.rem(me + by, n_fsdp)
            return lax.dynamic_index_in_dim(own_moe, dest, 0, keepdims=False)

        moe = for_block(0)
        for by in range(1, n_fsdp):
            moe = moe + shift(for_block(by).astype(bf16), by).astype(f32)
        own_state = lax.dynamic_slice(hstate, (me * block, group_index * run), (block, run))
        return (own_state.astype(f32) + moe).astype(bf16)

    return per_device


def solution(mesh):
    in_specs = (
        P(("groups", "fsdp"), "expert"),
        P(("groups", "fsdp"), None, "expert"),
        P(("groups", "fsdp"), None, "expert"),
        P("expert", "fsdp"),
        P(("groups", "fsdp"), None),
        P(),
        P(("groups", "fsdp"), None),
        P(("groups", "fsdp"), None),
        P(("groups", "fsdp"), None),
        P("expert", None, "fsdp"),
        P("expert", None, "fsdp"),
        P("expert", "fsdp", None),
    )
    out_specs = P(("groups", "fsdp"), "expert")
    return jax.shard_map(
        make_per_device(mesh.shape["fsdp"], mesh.shape["expert"]),
        mesh=mesh,
        in_specs=in_specs,
        out_specs=out_specs,
        check_vma=False,
    )
```
